32 devices in a mesh: data: 1 (over z), dap: 32 (over y, x, core).
Axes of the slice: x: 4, y: 4, z: 1, core: 2. Of those that a mesh axis runs over, the one named last changes fastest.
The devices are a block of a 4x4x8 slice.
Arguments:
- pair_act: float32 [256, 256, 128], P(('data', 'dap'))
- pair_mask: int32 [256, 256], P(('data', 'dap'))
- grad_out: float32 [256, 256, 128], P(('data', 'dap'))
- ln_pair: bfloat16 [2, 2, 128], replicated
- w_in: bfloat16 [2, 128, 640], replicated
- ln_tri: bfloat16 [2, 2, 128], replicated
- w_out: bfloat16 [2, 128, 128], replicated
Outputs:
- output 1: float32 [256, 256, 128], P(('data', 'dap'))
- output 2: float32 [2, 2, 128], P('data')
- output 3: float32 [2, 128, 640], P('data')
- output 4: float32 [2, 2, 128], P('data')
- output 5: float32 [2, 128, 128], P('data')
All inputs are finite; a program needn't handle non-finite values.
Results may differ from the reference program's by a relative error of at most 0.0148475.
Values are sent between devices in bfloat16 or wider.
A program may use at most 768 MiB of HBM per device.

```python
import jax
import jax.numpy as jnp
from jax import lax

PAIR_DIM = 128
HIDDEN = 128
ROWS_DEV = 8
GROUP_SIZE = 32
SEQ_LEN = ROWS_DEV * GROUP_SIZE
LN_EPS = 1e-5
OUT_FORM = 'ikc,jkc->ijc'
IN_FORM = 'kic,kjc->ijc'


def setup_inputs(seed: int = 0, part: int = 0) -> dict:
    part_keys = jax.random.split(jax.random.fold_in(jax.random.key(seed), part), 3)
    shared_keys = jax.random.split(jax.random.key(seed + 1), 6)
    width_in = 4 * HIDDEN + PAIR_DIM
    pair_act = jax.random.normal(part_keys[0], (SEQ_LEN, SEQ_LEN, PAIR_DIM), jnp.float32)
    tail_len = jax.random.randint(part_keys[1], (), SEQ_LEN // 16 + 1, SEQ_LEN // 8 + 2)
    seq_mask = (jnp.arange(SEQ_LEN) < SEQ_LEN - tail_len).astype(jnp.int32)
    pair_mask = seq_mask[:, None] * seq_mask[None, :]
    grad_out = jax.random.normal(part_keys[2], (SEQ_LEN, SEQ_LEN, PAIR_DIM), jnp.float32)
    gain_pair = 1.0 + 0.3 * jax.random.normal(shared_keys[0], (2, 1, PAIR_DIM), jnp.float32)
    bias_pair = 0.3 * jax.random.normal(shared_keys[1], (2, 1, PAIR_DIM), jnp.float32)
    w_in = jax.random.normal(shared_keys[2], (2, PAIR_DIM, width_in), jnp.float32) * PAIR_DIM ** -0.5
    gain_tri = 1.0 + 0.3 * jax.random.normal(shared_keys[3], (2, 1, HIDDEN), jnp.float32)
    bias_tri = 0.3 * jax.random.normal(shared_keys[4], (2, 1, HIDDEN), jnp.float32)
    w_out = jax.random.normal(shared_keys[5], (2, HIDDEN, PAIR_DIM), jnp.float32) * HIDDEN ** -0.5
    return {
        'pair_act': pair_act,
        'pair_mask': pair_mask,
        'grad_out': grad_out,
        'ln_pair': jnp.concatenate([gain_pair, bias_pair], axis=1).astype(jnp.bfloat16),
        'w_in': w_in.astype(jnp.bfloat16),
        'ln_tri': jnp.concatenate([gain_tri, bias_tri], axis=1).astype(jnp.bfloat16),
        'w_out': w_out.astype(jnp.bfloat16),
    }


def layer_norm(values, gain_vec, bias_vec):
    mean_val = jnp.mean(values, axis=-1, keepdims=True)
    centred = values - mean_val
    variance = jnp.mean(centred * centred, axis=-1, keepdims=True)
    return centred * lax.rsqrt(variance + LN_EPS) * gain_vec + bias_vec


def project_rows(row_vals, mask_rows, ln_pair, w_in):
    normed = layer_norm(row_vals, ln_pair[0], ln_pair[1]).astype(jnp.bfloat16)
    proj_all = jnp.einsum('ijc,cd->ijd', normed.astype(jnp.float32), w_in)
    mask_f = mask_rows.astype(jnp.float32)[:, :, None]
    left_act = (mask_f * jax.nn.sigmoid(proj_all[:, :, HIDDEN:2 * HIDDEN]) * proj_all[:, :, :HIDDEN]).astype(jnp.bfloat16)
    right_act = (mask_f * jax.nn.sigmoid(proj_all[:, :, 3 * HIDDEN:4 * HIDDEN]) * proj_all[:, :, 2 * HIDDEN:3 * HIDDEN]).astype(jnp.bfloat16)
    gate_act = jax.nn.sigmoid(proj_all[:, :, 4 * HIDDEN:])
    return left_act, right_act, gate_act


def finish_rows(row_vals, tri_sum, gate_act, ln_tri, w_out):
    tri_norm = layer_norm(tri_sum, ln_tri[0], ln_tri[1]).astype(jnp.bfloat16)
    return row_vals + gate_act * jnp.einsum('ijc,cd->ijd', tri_norm.astype(jnp.float32), w_out)


def tri_update(pair_act, pair_mask, ln_pair, w_in, ln_tri, w_out, ein_form):
    block_shape = (GROUP_SIZE, ROWS_DEV, SEQ_LEN)
    pair_blocks = pair_act.reshape(block_shape + (PAIR_DIM,))
    left_act, right_act, gate_act = lax.map(
        jax.checkpoint(lambda row_block: project_rows(row_block[0], row_block[1], ln_pair, w_in)),
        (pair_blocks, pair_mask.reshape(block_shape)))
    tri_sum = jnp.einsum(ein_form,
                         left_act.reshape(SEQ_LEN, SEQ_LEN, HIDDEN).astype(jnp.float32),
                         right_act.reshape(SEQ_LEN, SEQ_LEN, HIDDEN).astype(jnp.float32))
    new_blocks = lax.map(
        jax.checkpoint(lambda row_block: finish_rows(row_block[0], row_block[1], row_block[2], ln_tri, w_out)),
        (pair_blocks, tri_sum.reshape(block_shape + (HIDDEN,)), gate_act))
    return new_blocks.reshape(SEQ_LEN, SEQ_LEN, PAIR_DIM)


def block_forward(pair_act, pair_mask, ln_pair, w_in, ln_tri, w_out):
    mid_act = tri_update(pair_act, pair_mask, ln_pair[0], w_in[0], ln_tri[0], w_out[0], OUT_FORM)
    return tri_update(mid_act, pair_mask, ln_pair[1], w_in[1], ln_tri[1], w_out[1], IN_FORM)


def reference(pair_act, pair_mask, grad_out, ln_pair, w_in, ln_tri, w_out):
    def forward(pair_in, ln_pair_v, w_in_v, ln_tri_v, w_out_v):
        return block_forward(pair_in, pair_mask, ln_pair_v, w_in_v, ln_tri_v, w_out_v)
    pull_back = jax.vjp(forward, pair_act, ln_pair.astype(jnp.float32), w_in.astype(jnp.float32),
                        ln_tri.astype(jnp.float32), w_out.astype(jnp.float32))[1]
    grad_all = pull_back(grad_out)
    return (grad_all[0], grad_all[1], grad_all[2], grad_all[3], grad_all[4])
```

```python
import functools
import math

import jax
import jax.numpy as jnp
from jax import lax
from jax.experimental import pallas as pl
from jax.experimental.pallas import tpu as pltpu
from jax.sharding import PartitionSpec as P

LN_EPS = 1e-5
MESH = pl.DeviceIdType.MESH
F32 = jnp.float32
BF16 = jnp.bfloat16
LANES = 128
MESSAGES = 2

AB, X, DX, DAB, PAIR, SCATTER, GATHER, SHARE = range(8)


def dot_nn(lhs, rhs):
    return lax.dot_general(lhs, rhs, (((1,), (0,)), ((), ())), preferred_element_type=F32)


def dot_nt(lhs, rhs):
    return lax.dot_general(lhs, rhs, (((1,), (1,)), ((), ())), preferred_element_type=F32)


def norm_cols(values):
    mean_val = jnp.mean(values, axis=0, keepdims=True)
    centred = values - mean_val
    rstd = lax.rsqrt(jnp.mean(centred * centred, axis=0, keepdims=True) + LN_EPS)
    return centred * rstd, rstd


def norm_cols_back(d_out, normed, rstd, gain):
    d_hat = d_out * gain
    return rstd * (d_hat - jnp.mean(d_hat, axis=0, keepdims=True)
                   - normed * jnp.mean(d_hat * normed, axis=0, keepdims=True))


def body(n, rows, seq, dim,
         z_hbm, m_ref, go_hbm, lnp_ref, win_ref, lnt_ref, wout_ref,
         gp_hbm, early_hbm, late_hbm, ln_hbm,
         z_ref, go_ref, gp_ref, stg, ab_s, r_ab, ch, x_s, x_r, dx_s, r_dx, dab_s, r_dab,
         z_t, go_t, d_mid, xh_p, rs_p, zn_b, fac, gate, y0, xh_t, rs_t, xn_b, dpr_b, d_cat,
         w_t, wo_t, gb, mf, acc, e_acc, e_part, e_pair, e_half, e_recv, e_sum, e_all,
         l_acc, l_part, l_pair, l_half, l_recv, l_sum, ln_part,
         send_sem, recv_sem, local_sem):
    chans = dim // n
    chunk = chans * rows
    wide = win_ref.shape[2]
    blocks = wide // dim
    e_rows = e_recv.shape[1]
    halves = seq // LANES
    pairs = MESSAGES
    held = chans // pairs
    part = held * rows
    per = seq // LANES
    slabs = rows // per
    me = lax.axis_index('dap')
    core = me & 1
    chip = lax.shift_right_logical(me, 1)
    chips = n // 2

    def tag(kind, u, h=0, p=0):
        if kind >= PAIR:
            return 8 * halves * pairs + 4 * u + kind - PAIR
        return ((2 * kind + u) * halves + h) * pairs + p

    def start_all(parts):
        def one(dst):
            for group, src, slot in parts:
                pltpu.make_async_remote_copy(
                    src_ref=src(dst), dst_ref=slot, send_sem=send_sem.at[group],
                    recv_sem=recv_sem.at[group], device_id={'dap': dst}, device_id_type=MESH).start()
        each_peer(one)

    def each_peer(one):
        if n != 32:
            def step(k, carry):
                one(lax.rem(me + 1 + k, n))
                return carry
            lax.fori_loop(0, n - 1, step, 0)
            return
        def line(chip_y, offsets):
            for off in offsets:
                chip_x = (lax.shift_right_logical(me, 1) + off) & 3
                for c in (0, 1):
                    one(chip_y * 8 + chip_x * 2 + ((me + c) & 1))
        mine_y = lax.shift_right_logical(me, 3)
        def step(k, carry):
            off = 2 - k + 4 * lax.shift_right_logical(k, 1) - lax.shift_right_logical(k, 1)
            line((mine_y + off) & 3, (2, 1, 3, 0))
            return carry
        lax.fori_loop(0, 3, step, 0)
        line(mine_y, (2, 1, 3))
        one(me + 1 - 2 * (me & 1))

    def partner(group, src, dst):
        return pltpu.make_async_remote_copy(
            src_ref=src, dst_ref=dst, send_sem=send_sem.at[group], recv_sem=recv_sem.at[group],
            device_id={'dap': me + 1 - 2 * core}, device_id_type=MESH)

    def chip_at(k):
        if chips != 16:
            return lax.rem(chip + 1 + k, chips)
        def far_first(unit):
            top = lax.shift_right_logical(unit, 1)
            return 2 - unit + 3 * top + 2 * (unit & top)
        chip_y = (lax.shift_right_logical(chip, 2) + far_first(lax.shift_right_logical(k, 2))) & 3
        return chip_y * 4 + ((chip + far_first(k & 3)) & 3)

    def start_chips(group, src, slot):
        def step(k, carry):
            dst = chip_at(k)
            pltpu.make_async_remote_copy(
                src_ref=src(dst), dst_ref=slot, send_sem=send_sem.at[group], recv_sem=recv_sem.at[group],
                device_id={'dap': 2 * dst + core}, device_id_type=MESH).start()
            return carry
        lax.fori_loop(0, chips - 1, step, 0)

    def whole(group, ref):
        view = ref.at[pl.ds(0, ref.shape[0] - 1)]
        return pltpu.make_async_remote_copy(
            src_ref=view, dst_ref=view, send_sem=send_sem.at[group], recv_sem=recv_sem.at[group],
            device_id={'dap': me}, device_id_type=MESH)

    def wait_all(group, ref):
        whole(group, ref).wait_recv()

    def wait_sent(group, ref):
        whole(group, ref).wait_send()

    def for_slabs(half, fn):
        def step(q, carry):
            fn(half * slabs + q, half, q)
            return carry
        lax.fori_loop(0, slabs, step, 0)

    def row_of(i):
        return pl.ds(i, dim, stride=rows)

    def put_slab(stage, q, vals):
        for r in range(per):
            stage[row_of(per * q + r), :] = vals[:, r * LANES:(r + 1) * LANES]

    def get_slab(stage, q):
        return jnp.concatenate([stage[row_of(per * q + r), :] for r in range(per)], axis=1)

    def turned(ref, half, q):
        return jnp.concatenate(
            [ref[per * q + r, pl.ds(half * LANES, LANES), :].T for r in range(per)], axis=1)

    def chan_pair(parts):
        both = [block.astype(F32) for block in parts]
        return [jnp.concatenate([b[:, k * rows:(k + 1) * rows, :].reshape(seq, LANES) for b in both], axis=1)
                for k in range(held)]

    def half_of(vals, h):
        return jnp.concatenate([v[:, h * LANES:(h + 1) * LANES].reshape(n, rows, LANES) for v in vals], axis=1)

    def by_pair(stage):
        both = stage[...].astype(BF16).reshape(n, chunk, LANES)
        return [both[:, p * part:(p + 1) * part] for p in range(pairs)]

    def lanes_of(q):
        return pl.ds(pl.multiple_of(q * per * LANES, per * LANES), per * LANES)

    def half_in(h):
        cols = pl.ds(h * LANES, LANES)
        return pltpu.make_async_copy(z_hbm.at[:, cols, :], z_ref.at[:, cols, :], local_sem.at[2 + h])
    for h in range(halves):
        half_in(h).start()
    grad_in = pltpu.make_async_copy(go_hbm, go_ref, local_sem.at[0])
    grad_in.start()

    barrier = pltpu.get_barrier_semaphore()
    with jax.named_scope('each_peer_lambda_dst_pl'):
        each_peer(lambda dst: pl.semaphore_signal(barrier, inc=1, device_id={'dap': dst}, device_id_type=MESH))

    def columns(ref, u, k):
        return jnp.broadcast_to(ref[u, pl.ds(k, 1), :].astype(F32), (seq, dim)).T
    def prepare(u):
        for k in range(2):
            gb[u, k] = columns(lnp_ref, u, k)
        w_t[u] = win_ref[u].astype(F32).T.astype(BF16)
    def prepare_out(u):
        for k in range(2):
            gb[u, 2 + k] = columns(lnt_ref, u, k)
        wo_t[u] = wout_ref[u].astype(F32).T.astype(BF16)
    with jax.named_scope('prepare_0'):
        prepare(0)
    mask = m_ref[...].astype(F32)
    for h in range(halves):
        for q in range(slabs):
            for r in range(per):
                mf[pl.ds(h * slabs + q, 1), pl.ds(r * LANES, LANES)] = (
                    mask[per * q + r:per * q + r + 1, h * LANES:(h + 1) * LANES])

    def project(s, u, h, q, rows_t):
        normed, rstd = norm_cols(rows_t)
        zn = (normed * gb[u, 0] + gb[u, 1]).astype(BF16)
        xh_p[u, s] = normed
        rs_p[u, pl.ds(s, 1), :] = rstd
        zn_b[u, h, :, lanes_of(q)] = zn
        proj = dot_nn(w_t[u], zn)
        mask = mf[pl.ds(s, 1), :]
        for k in range(2):
            lin = proj[2 * k * dim:(2 * k + 1) * dim]
            sig = jax.nn.sigmoid(proj[(2 * k + 1) * dim:(2 * k + 2) * dim])
            msig = mask * sig
            act = msig * lin
            put_slab(stg.at[k], q, act)
            fac[u, 2 * k, s] = msig
            fac[u, 2 * k + 1, s] = act * (1.0 - sig)
        gate[u, s] = jax.nn.sigmoid(proj[4 * dim:])

    def send_ab(u, h):
        parts = [by_pair(stg.at[k]) for k in range(2)]
        for p in range(pairs):
            for k in range(2):
                ab_s[u, h, p, :, k] = parts[k][p]
            start_all([(tag(AB, u, h, p), lambda d: ab_s.at[u, h, p, d], r_ab.at[u, h, p, me])])
        for p in range(pairs):
            r_ab[u, h, p, me] = ab_s[u, h, p, me]

    def finish(s, u, h, q):
        normed, rstd = norm_cols(get_slab(x_r.at[u, h], q))
        xn = (normed * gb[u, 2] + gb[u, 3]).astype(BF16)
        xn_b[u, h, :, lanes_of(q)] = xn
        return normed, rstd, dot_nn(wo_t[u], xn)

    def finish_back(s, u, h, q, d_new, normed, rstd, proj_out):
        gate_v = gate[u, s]
        d_g = d_new * gate_v
        d_cat[u, h, pl.ds(4 * dim, dim), lanes_of(q)] = (d_g * proj_out * (1.0 - gate_v)).astype(BF16)
        d_proj = d_g.astype(BF16)
        dpr_b[u, h, :, lanes_of(q)] = d_proj
        d_norm = dot_nn(wout_ref[u], d_proj).astype(BF16).astype(F32)
        acc[u, 2] += d_norm * normed
        acc[u, 3] += d_norm
        put_slab(stg.at[2], q, norm_cols_back(d_norm, normed, rstd, gb[u, 2]))

    def send_dx(u, h):
        dx_s[u, h] = stg[2].astype(BF16).reshape(n, chunk, LANES)
        start_all([(tag(DX, u, h), lambda d: dx_s.at[u, h, d], r_dx.at[u, h, me])])
        r_dx[u, h, me] = dx_s[u, h, me]

    def put_x(u, p, vals):
        own = pl.ds(pl.multiple_of(chunk * me + part * p, part), part)
        for h in range(halves):
            x_s[u, h, p] = half_of(vals, h)
            x_r[u, h, own, :] = x_s[u, h, p, me]

    def start_x(u, h, p):
        own = pl.ds(pl.multiple_of(chunk * me + part * p, part), part)
        start_all([(tag(X, u, h, p), lambda d: x_s.at[u, h, p, d], x_r.at[u, h, own, :])])

    def rest(u, start, kind, src):
        for h in range(1, halves):
            for p in range(pairs):
                wait_sent(tag(kind, u, h - 1, p), src.at[u, h - 1, p])
                start(u, h, p)

    def take_x(u, h):
        for p in range(pairs):
            wait_all(tag(X, u, h, p), x_s.at[u, h, p])

    def put_dab(u, p, d_a, d_b):
        for h in range(halves):
            for k, vals in enumerate((d_a, d_b)):
                dab_s[u, h, p, :, k] = half_of(vals, h).astype(BF16)
            r_dab[u, h, p, me] = dab_s[u, h, p, me]

    def start_dab(u, h, p):
        start_all([(tag(DAB, u, h, p), lambda d: dab_s.at[u, h, p, d], r_dab.at[u, h, p, me])])

    def take_dab(u, h):
        for p in range(pairs):
            wait_all(tag(DAB, u, h, p), r_dab.at[u, h, p])
        for k in range(2):
            both = jnp.concatenate([r_dab[u, h, p, :, k].astype(F32) for p in range(pairs)], axis=1)
            stg[k] = both.reshape(n * chunk, LANES)

    def cat_slab(s, u, h, q):
        for k in range(2):
            val = get_slab(stg.at[k], q)
            for j in (2 * k, 2 * k + 1):
                d_cat[u, h, pl.ds(j * dim, dim), lanes_of(q)] = (val * fac[u, j, s]).astype(BF16)

    def project_back(s, u, h, q):
        d_zn = dot_nn(win_ref[u], d_cat[u, h, :, lanes_of(q)]).astype(BF16).astype(F32)
        normed = xh_p[u, s]
        acc[u, 0] += d_zn * normed
        acc[u, 1] += d_zn
        return norm_cols_back(d_zn, normed, rs_p[u, pl.ds(s, 1), :], gb[u, 0])

    def early_grads(h):
        tops = ((d_cat.at[1], zn_b.at[1], 0, wide), (dpr_b.at[1], xn_b.at[1], wide, dim),
                (dpr_b.at[0], xn_b.at[0], wide + dim, dim), (d_cat.at[0], zn_b.at[0], wide + 2 * dim, dim))
        def add(s, h, q):
            for k, (left, right, top, count) in enumerate(tops):
                rows_of = pl.ds(4 * dim, dim) if k == 3 else pl.ds(0, count)
                e_acc[pl.ds(top, count), :] += dot_nt(left[h, rows_of, lanes_of(q)], right[h, :, lanes_of(q)])
        with jax.named_scope('for_slabs_h_add'):
            for_slabs(h, add)

    def late_slab(s, h, q):
        cat_slab(s, 0, h, q)
        l_acc[...] += dot_nt(d_cat[0, h, pl.ds(0, 4 * dim), lanes_of(q)], zn_b[0, h, :, lanes_of(q)])

    def pair_grads(u, acc_ref, part_ref, pair_ref):
        part_ref[...] = acc_ref[...].reshape(part_ref.shape)
        partner(tag(PAIR, u), part_ref.at[1 - core], pair_ref).start()

    def scatter_grads(u, part_ref, pair_ref, half_ref, recv_ref):
        partner(tag(PAIR, u), part_ref.at[1 - core], pair_ref).wait_recv()
        half_ref[...] = part_ref[core] + pair_ref[...]
        start_chips(tag(SCATTER, u), lambda d: half_ref.at[d], recv_ref.at[chip])
        recv_ref[chip] = half_ref[chip]

    def gather_early():
        with jax.named_scope('wait_all_tag_SCATTER_1'):
            wait_all(tag(SCATTER, 1), e_recv)
        e_sum[...] = jnp.sum(e_recv[...], axis=0)
        start_chips(tag(GATHER, 1), lambda d: e_sum, e_all.at[core, chip])
        e_all[core, chip] = e_sum[...]

    def share_early():
        with jax.named_scope('wait_all_tag_GATHER_1_e'):
            wait_all(tag(GATHER, 1), e_all.at[0])
        partner(tag(SHARE, 1), e_all.at[core], e_all.at[core]).start()

    late_own = pltpu.make_async_copy(l_sum, late_hbm.at[core * chips + chip], local_sem.at[0])

    def gather_late():
        with jax.named_scope('wait_all_tag_SCATTER_0'):
            wait_all(tag(SCATTER, 0), l_recv)
        l_sum[...] = jnp.sum(l_recv[...], axis=0)
        start_all([(tag(GATHER, 0), lambda d: l_sum, late_hbm.at[core * chips + chip])])
        late_own.start()

    def first(s, h, q):
        rows_t = turned(z_ref, h, q)
        z_t[s] = rows_t
        project(s, 0, h, q, rows_t)

    def second(s, h, q):
        normed, rstd, proj_out = finish(s, 0, h, q)
        xh_t[s] = normed
        rs_t[pl.ds(s, 1), :] = rstd
        y0[s] = proj_out
        project(s, 1, h, q, z_t[s] + gate[0, s] * proj_out)

    def third(s, h, q):
        normed, rstd, proj_out = finish(s, 1, h, q)
        finish_back(s, 1, h, q, go_t[s], normed, rstd, proj_out)

    def fourth(s, h, q):
        cat_slab(s, 1, h, q)
        d_rows = go_t[s] + project_back(s, 1, h, q)
        d_mid[s] = d_rows
        finish_back(s, 0, h, q, d_rows, xh_t[s], rs_t[pl.ds(s, 1), :], y0[s])

    def turn(s, h, q):
        go_t[s] = turned(go_ref, h, q)

    def last(s, h, q):
        d_rows = d_mid[s] + project_back(s, 0, h, q)
        for r in range(per):
            gp_ref[per * q + r, pl.ds(h * LANES, LANES), :] = d_rows[:, r * LANES:(r + 1) * LANES].T

    def ab_pair(u, p):
        for h in range(halves):
            wait_all(tag(AB, u, h, p), r_ab.at[u, h, p])
        return zip(*[chan_pair([r_ab[u, h, p, :, k] for h in range(halves)]) for k in range(2)])

    def take_dx(u):
        for h in range(halves):
            wait_all(tag(DX, u, h), r_dx.at[u, h])

    def dx_pair(u, p):
        return chan_pair([r_dx[u, h, :, pl.ds(p * part, part), :] for h in range(halves)])

    for h in range(halves):
        half_in(h).wait()
        with jax.named_scope('for_slabs_h_first'):
            for_slabs(h, first)
        if h == 0:
            pl.semaphore_wait(barrier, n - 1)
        with jax.named_scope('send_ab_0_h'):
            send_ab(0, h)
    with jax.named_scope('prepare_out_0'):
        prepare_out(0)
    with jax.named_scope('prepare_1'):
        prepare(1)
    with jax.named_scope('prepare_out_1'):
        prepare_out(1)
    acc[...] = jnp.zeros_like(acc)
    e_acc[...] = jnp.zeros_like(e_acc)
    l_acc[...] = jnp.zeros_like(l_acc)
    grad_in.wait()
    for h in range(halves):
        with jax.named_scope('for_slabs_h_turn'):
            for_slabs(h, turn)

    for p in range(pairs):
        out = []
        for k, (left, right) in enumerate(ab_pair(0, p)):
            left, right = left.astype(BF16), right.astype(BF16)
            ch[0, 0, held * p + k] = left
            ch[0, 1, held * p + k] = right
            out.append(dot_nt(left, right))
        put_x(0, p, out)
        start_x(0, 0, p)
    rest(0, start_x, X, x_s)

    for h in range(halves):
        with jax.named_scope('take_x_0_h'):
            take_x(0, h)
        with jax.named_scope('for_slabs_h_second'):
            for_slabs(h, second)
        with jax.named_scope('send_ab_1_h'):
            send_ab(1, h)

    for p in range(pairs):
        out = []
        for k, (left, right) in enumerate(ab_pair(1, p)):
            right = right.astype(BF16)
            ch[1, 0, held * p + k] = left.astype(BF16)
            ch[1, 1, held * p + k] = right
            out.append(dot_nn(left.T.astype(BF16), right))
        put_x(1, p, out)
        start_x(1, 0, p)
    rest(1, start_x, X, x_s)

    for h in range(halves):
        with jax.named_scope('take_x_1_h'):
            take_x(1, h)
        with jax.named_scope('for_slabs_h_third'):
            for_slabs(h, third)
        with jax.named_scope('send_dx_1_h'):
            send_dx(1, h)

    with jax.named_scope('take_dx_1'):
        take_dx(1)
    for p in range(pairs):
        out_a, out_b = [], []
        for k, d_x in enumerate(dx_pair(1, p)):
            d_x = d_x.astype(BF16)
            out_a.append(dot_nt(ch[1, 1, held * p + k], d_x))
            out_b.append(dot_nn(ch[1, 0, held * p + k], d_x))
        put_dab(1, p, out_a, out_b)
        start_dab(1, 0, p)
    rest(1, start_dab, DAB, dab_s)

    for h in range(halves):
        with jax.named_scope('take_dab_1_h'):
            take_dab(1, h)
        with jax.named_scope('for_slabs_h_fourth'):
            for_slabs(h, fourth)
        with jax.named_scope('send_dx_0_h'):
            send_dx(0, h)
        with jax.named_scope('early_grads_h'):
            early_grads(h)
    with jax.named_scope('pair_grads_1_e_acc_e_part'):
        pair_grads(1, e_acc, e_part, e_pair)
    with jax.named_scope('scatter_grads_1_e_part_e_pai'):
        scatter_grads(1, e_part, e_pair, e_half, e_recv)

    with jax.named_scope('take_dx_0'):
        take_dx(0)
    for p in range(pairs):
        out_a, out_b = [], []
        for k, d_x in enumerate(dx_pair(0, p)):
            d_xt = d_x.T.astype(BF16)
            out_a.append(dot_nn(d_x.astype(BF16), ch[0, 1, held * p + k]))
            out_b.append(dot_nn(d_xt, ch[0, 0, held * p + k]))
        put_dab(0, p, out_a, out_b)
        start_dab(0, 0, p)
    rest(0, start_dab, DAB, dab_s)

    for h in range(halves):
        with jax.named_scope('take_dab_0_h'):
            take_dab(0, h)
        with jax.named_scope('for_slabs_h_late_slab'):
            for_slabs(h, late_slab)
        if h == halves - 1:
            pair_grads(0, l_acc, l_part, l_pair)
            gather_early()
        with jax.named_scope('for_slabs_h_last'):
            for_slabs(h, last)
    with jax.named_scope('scatter_grads_0_l_part_l_pai'):
        scatter_grads(0, l_part, l_pair, l_half, l_recv)
    grad_out = pltpu.make_async_copy(gp_ref, gp_hbm, local_sem.at[1])
    grad_out.start()
    for u in range(2):
        for k in range(4):
            val = acc[u, k]
            val = sum(val[:, s:s + dim] for s in range(0, seq, dim))
            ln_part[pl.ds(4 * u + k, 1), :] = jnp.sum(val.T, axis=0, keepdims=True)
    start_all([(tag(SHARE, 0), lambda d: ln_part, ln_hbm.at[me])])
    ln_own = pltpu.make_async_copy(ln_part, ln_hbm.at[me], local_sem.at[3])
    ln_own.start()
    share_early()
    gather_late()
    partner(tag(SHARE, 1), e_all.at[core], e_all.at[1 - core]).wait_recv()
    early_out = pltpu.make_async_copy(e_all, early_hbm, local_sem.at[2])
    early_out.start()
    with jax.named_scope('wait_all_tag_GATHER_0_l'):
        wait_all(tag(GATHER, 0), late_hbm)
    late_own.wait()
    with jax.named_scope('wait_all_tag_SHARE_0_ln'):
        wait_all(tag(SHARE, 0), ln_hbm)
    ln_own.wait()
    early_out.wait()
    grad_out.wait()
    for u in range(2):
        for h in range(halves):
            for p in range(pairs):
                wait_sent(tag(AB, u, h, p), ab_s.at[u, h, p])
                if p == 0:
                    wait_sent(tag(DX, u, h), dx_s.at[u, h])
                if h == halves - 1:
                    wait_sent(tag(X, u, h, p), x_s.at[u, h, p])
                    wait_sent(tag(DAB, u, h, p), dab_s.at[u, h, p])
    partner(tag(PAIR, 0), l_part.at[1 - core], l_pair).wait_send()
    partner(tag(PAIR, 1), e_part.at[1 - core], e_pair).wait_send()
    with jax.named_scope('wait_sent_tag_SCATTER_0'):
        wait_sent(tag(SCATTER, 0), l_half)
    with jax.named_scope('wait_sent_tag_SCATTER_1'):
        wait_sent(tag(SCATTER, 1), e_half)
    with jax.named_scope('wait_sent_tag_GATHER_0_l'):
        wait_sent(tag(GATHER, 0), late_hbm)
    with jax.named_scope('wait_sent_tag_SHARE_0_ln'):
        wait_sent(tag(SHARE, 0), ln_hbm)
    with jax.named_scope('wait_sent_tag_GATHER_1_e'):
        wait_sent(tag(GATHER, 1), e_all.at[0])
    partner(tag(SHARE, 1), e_all.at[core], e_all.at[core]).wait_send()


def move_out(dim, gp_in, early_in, late_in, ln_in, gp_out, glnp_out, gwin_out, glnt_out, gwout_out,
             gp_buf, early, late, ln, glnp, gwin, glnt, gwout, in_sem, out_sem):
    steps = in_sem.shape[0] - 3
    rows = gp_buf.shape[0] // steps
    ins = [pltpu.make_async_copy(src, dst, in_sem.at[steps + k])
           for k, (src, dst) in enumerate(((early_in, early), (late_in, late), (ln_in, ln)))]
    views = [pl.ds(k * rows, rows) for k in range(steps)]
    moves_in = [pltpu.make_async_copy(gp_in.at[v], gp_buf.at[v], in_sem.at[k]) for k, v in enumerate(views)]
    moves_out = [pltpu.make_async_copy(gp_buf.at[v], gp_out.at[v], out_sem.at[k]) for k, v in enumerate(views)]
    for copy in ins + moves_in:
        copy.start()
    for copy in ins:
        copy.wait()
    blocks = gwin.shape[2] // dim
    early_rows = early[...].reshape(-1, dim)
    late_rows = late[...].reshape(-1, dim)
    ln_sum = jnp.sum(ln[...], axis=0)
    def block(rows_t, k):
        return rows_t[k * dim:(k + 1) * dim].T
    for k in range(blocks):
        cols = pl.ds(k * dim, dim)
        gwin[1, :, cols] = block(early_rows, k)
        gwin[0, :, cols] = block(late_rows, k) if k < blocks - 1 else block(early_rows, blocks + 2)
    gwout[1] = block(early_rows, blocks)
    gwout[0] = block(early_rows, blocks + 1)
    for u in range(2):
        glnp[u] = ln_sum[4 * u:4 * u + 2]
        glnt[u] = ln_sum[4 * u + 2:4 * u + 4]
    outs = [pltpu.make_async_copy(src, dst, out_sem.at[steps + k]) for k, (src, dst) in enumerate(
        ((gwin, gwin_out), (gwout, gwout_out), (glnp, glnp_out), (glnt, glnt_out)))]
    for copy in outs:
        copy.start()
    for copy, out in zip(moves_in, moves_out):
        copy.wait()
        out.start()
    for out in moves_out + outs:
        out.wait()


def solution(mesh):
    row_spec = P(('data', 'dap'))
    grad_spec = P('data')
    n = mesh.shape['dap']

    def device_body(pair_act, pair_mask, grad_out, ln_pair, w_in, ln_tri, w_out):
        rows, seq, dim = pair_act.shape
        wide = w_in.shape[2]
        chans = dim // n
        chunk = chans * rows
        e_rows = (wide + 3 * dim) // n
        l_rows = (wide - dim) // n
        chips = n // 2
        pairs = MESSAGES
        part = chunk // pairs
        halves = seq // LANES
        slabs = halves * (rows // (seq // LANES))
        groups = 8 * halves * pairs + 8
        half = slabs // halves * (seq * rows // slabs)
        vmem = pltpu.VMEM
        slab = (slabs, dim, seq * rows // slabs)
        line = (slabs, seq * rows // slabs)
        scratch = [
            vmem(grad_out.shape, F32), vmem(grad_out.shape, F32), vmem(grad_out.shape, F32),
            vmem((3, n * chunk, LANES), F32),
            vmem((2, halves, pairs, n, 2, part, LANES), BF16), vmem((2, halves, pairs, n, 2, part, LANES), BF16),
            vmem((2, 2, chans, seq, seq), BF16),
            vmem((2, halves, pairs, n, part, LANES), F32), vmem((2, halves, n * chunk, LANES), F32),
            vmem((2, halves, n, chunk, LANES), BF16), vmem((2, halves, n, chunk, LANES), BF16),
            vmem((2, halves, pairs, n, 2, part, LANES), BF16), vmem((2, halves, pairs, n, 2, part, LANES), BF16),
            vmem(slab, F32), vmem(slab, F32), vmem(slab, F32),
            vmem((2,) + slab, F32), vmem((2,) + line, F32), vmem((2, halves, dim, half), BF16),
            vmem((2, 4) + slab, F32), vmem((2,) + slab, F32),
            vmem(slab, F32), vmem(slab, F32), vmem(line, F32),
            vmem((2, halves, dim, half), BF16), vmem((2, halves, dim, half), BF16), vmem((2, halves, wide, half), BF16),
            vmem((2, wide, dim), BF16), vmem((2, dim, dim), BF16), vmem((2, 4, dim, seq), F32),
            vmem(line, F32), vmem((2, 4, dim, seq), F32),
            vmem((n * e_rows, dim), F32), vmem((2, chips, e_rows, dim), F32), vmem((chips, e_rows, dim), F32),
            vmem((chips, e_rows, dim), F32), vmem((chips, e_rows, dim), F32), vmem((e_rows, dim), F32),
            vmem((2, chips, e_rows, dim), F32),
            vmem((n * l_rows, dim), F32), vmem((2, chips, l_rows, dim), F32), vmem((chips, l_rows, dim), F32),
            vmem((chips, l_rows, dim), F32), vmem((chips, l_rows, dim), F32), vmem((l_rows, dim), F32), vmem((8, dim), F32),
            pltpu.SemaphoreType.DMA((groups,)), pltpu.SemaphoreType.DMA((groups,)),
            pltpu.SemaphoreType.DMA((2 + halves,)),
        ]
        hold = pl.BlockSpec(memory_space=vmem)
        free = pl.BlockSpec(memory_space=pl.ANY)
        shapes = [jax.ShapeDtypeStruct(v.shape, F32) for v in (pair_act, ln_pair, w_in, ln_tri, w_out)]
        early_shape = (2, chips, e_rows, dim)
        late_shape = (n, l_rows, dim)
        ln_shape = (n, 8, dim)
        results = pl.pallas_call(
            functools.partial(body, n, rows, seq, dim),
            name='triangle_backward',
            out_shape=[shapes[0], jax.ShapeDtypeStruct(early_shape, F32), jax.ShapeDtypeStruct(late_shape, F32),
                       jax.ShapeDtypeStruct(ln_shape, F32)],
            in_specs=[free, hold, free, hold, hold, hold, hold],
            out_specs=[free] * 4,
            scratch_shapes=scratch,
            compiler_params=pltpu.CompilerParams(
                collective_id=0, has_side_effects=True, vmem_limit_bytes=67043328),
        )(pair_act, pair_mask, grad_out, ln_pair, w_in, ln_tri, w_out)
        return pl.pallas_call(
            functools.partial(move_out, dim),
            name='move_out',
            out_shape=shapes,
            in_specs=[free] * 4,
            out_specs=[free] * 5,
            scratch_shapes=[vmem(shapes[0].shape, F32), vmem(early_shape, F32), vmem(late_shape, F32), vmem(ln_shape, F32)]
            + [vmem(v.shape, F32) for v in shapes[1:]]
            + [pltpu.SemaphoreType.DMA((7,)), pltpu.SemaphoreType.DMA((8,))],
        )(*results)

    return jax.shard_map(device_body, mesh=mesh,
                         in_specs=(row_spec, row_spec, row_spec, P(), P(), P(), P()),
                         out_specs=(row_spec, grad_spec, grad_spec, grad_spec, grad_spec),
                         check_vma=False)
```
